32 devices in a mesh: gx: 4 (over y, core), gy: 4 (over z), gz: 2 (over x).
Axes of the slice: x: 2, y: 2, z: 4, core: 2. Of those that a mesh axis runs over, the one named last changes fastest.
Arguments:
- fractions: float32 [3, 4, 8, 4, 128], P(None, 'gx', 'gy', 'gz'), may hold values from 0 to 1
- polarizability: float32 [4, 8, 4, 128], P('gx', 'gy', 'gz'), may hold values from 0.5 to 2
- occupancy: int32 [4, 8, 4, 128], P('gx', 'gy', 'gz'), may hold values 0 or 1
- pair_mask: int32 [4, 8, 4, 27], P('gx', 'gy', 'gz'), may hold values from 0 to 1, as said below
- perm_field: float32 [6, 4, 8, 4, 128], P(None, 'gx', 'gy', 'gz'), may hold values from -6 to 6
- history: float32 [6, 6, 4, 8, 4, 128], P(None, None, 'gx', 'gy', 'gz'), may hold values from -12 to 12
Outputs:
- induced: float32 [6, 4, 8, 4, 128], P(None, 'gx', 'gy', 'gz')
- change: float32 [], replicated
The draws below stay inside these ranges and needn't reach their ends.
Inputs may be any that keep to these rules, and one draw needn't show every extreme that they name: pair_mask[t, k] equals pair_mask at tile t + offset(k) for the opposite offset 26 - k (periodic); pair_mask[t, 13] (the tile itself) is 1.
All inputs are finite; a program needn't handle non-finite values. No bound on the sum of `occupancy` on one device may be relied on, other than what follows from the above.
Results may differ from the reference program's by a relative error of at most 0.0003.
Values sent between devices are 32-bit elements; how exact they have to be, the bound alone decides.
A program may use at most 64 MiB of HBM per device.

```python
import math
import jax
import jax.numpy as jnp
from jax import lax

TILE = 128
HIST = 6
TILES_X = 1
TILES_Y = 2
TILES_Z = 2
BOX_X = 4
BOX_Y = 8
BOX_Z = 4


def draw_history(key, part):
    subkeys = jax.random.split(key, 6)
    full_shape = (6, BOX_X, BOX_Y, BOX_Z, TILE)
    block_counts = (BOX_X // TILES_X, BOX_Y // TILES_Y, BOX_Z // TILES_Z)
    frequency_table = jax.random.uniform(subkeys[4], block_counts, jnp.float32, 0.25, 2.2)
    index_x = jnp.arange(BOX_X) // TILES_X
    index_y = jnp.arange(BOX_Y) // TILES_Y
    index_z = jnp.arange(BOX_Z) // TILES_Z
    frequency = frequency_table[index_x[:, None, None], index_y[None, :, None], index_z[None, None, :]]
    step_index = jnp.arange(HIST, dtype=jnp.float32).reshape(HIST, 1, 1, 1, 1, 1)
    phase_angle = step_index * frequency[None, None, :, :, :, None]
    baseline = jax.random.normal(subkeys[0], full_shape, jnp.float32)
    cosine_part = jax.random.normal(subkeys[1], full_shape, jnp.float32)
    sine_part = jax.random.normal(subkeys[2], full_shape, jnp.float32)
    jitter = 0.2 * jax.random.normal(subkeys[3], (HIST,) + full_shape, jnp.float32)
    amplitude = jnp.exp(jax.random.uniform(subkeys[5], (1, 1, BOX_X, BOX_Y, BOX_Z, 1), jnp.float32, -0.7, 0.7))
    values = amplitude * (baseline[None] + jnp.cos(phase_angle) * cosine_part[None] + jnp.sin(phase_angle) * sine_part[None] + jitter)
    return jnp.clip(values, -12.0, 12.0).astype(jnp.float32)


def draw_pair_mask(key, part):
    coin_flips = jax.random.randint(key, (BOX_X, BOX_Y, BOX_Z, 27), 0, 4)
    one_side = (coin_flips > 0).astype(jnp.int32)
    columns = []
    for offset in range(27):
        along_x = offset // 9 - 1
        along_y = offset // 3 % 3 - 1
        along_z = offset % 3 - 1
        if offset == 13:
            columns.append(jnp.ones_like(one_side[..., offset]))
        else:
            mirror = jnp.roll(one_side[..., 26 - offset], shift=(-along_x, -along_y, -along_z), axis=(0, 1, 2))
            columns.append(one_side[..., offset] * mirror)
    return jnp.stack(columns, -1).astype(jnp.int32)


def with_ends(drawn, own_key, low, top_value):
    extent = drawn.shape
    index_at = [jax.random.randint(jax.random.fold_in(own_key, axis), (), 0, extent[axis]) for axis in range(len(extent))]
    drawn = drawn.at[tuple(index_at)].set(low)
    longest = extent.index(max(extent))
    index_at[longest] = (index_at[longest] + 1) % extent[longest]
    return drawn.at[tuple(index_at)].set(top_value)


def shard_levels(key, extent, cuts, least, high):
    loudness = 1.0
    for axis_at, blocks in cuts:
        draws = jax.random.uniform(jax.random.fold_in(jax.random.fold_in(key, 6), axis_at), (blocks,), jnp.float32, least / len(cuts), high / len(cuts))
        loudness = loudness * jnp.repeat(jnp.exp(draws), extent[axis_at] // blocks).reshape((-1,) + (1,) * (len(extent) - 1 - axis_at))
    return loudness


def scatter_about(key, dims, width, limit, pieces=(), held_as=jnp.bfloat16):
    result = jax.random.normal(key, dims, jnp.float32) * width
    if len(pieces) > 0:
        result = shard_levels(key, dims, pieces, -0.22, 0.18) * result
    return jnp.clip(result, min=-limit, max=limit).astype(held_as)


def setup_inputs(seed: int = 0) -> dict:
    key_of = jax.random.split(jax.random.key(seed), 7)
    fractions = jnp.clip(1.0 * jax.random.uniform(key_of[0], (3, BOX_X, BOX_Y, BOX_Z, TILE), jnp.float32) ** shard_levels(key_of[0], (3, BOX_X, BOX_Y, BOX_Z, TILE), ((1, 4), (2, 4), (3, 2)), -0.2, 0.2), 0.0, 1.0)
    polarizability = jnp.clip(jnp.exp(math.log(2.0) - 1.3862944 * jax.random.uniform(key_of[1], (BOX_X, BOX_Y, BOX_Z, TILE), jnp.float32) ** shard_levels(key_of[1], (BOX_X, BOX_Y, BOX_Z, TILE), ((0, 4), (1, 4), (2, 2)), -0.2, 0.2)), 0.5, 2.0)
    occupancy = with_ends((jax.random.randint(key_of[2], (BOX_X, BOX_Y, BOX_Z, TILE), 0, 8) < 7).astype(jnp.int32), jax.random.fold_in(key_of[2], 1), 0, 1)
    pair_mask = draw_pair_mask(jax.random.fold_in(key_of[6], 71), 0)
    perm_field = scatter_about(key_of[4], (6, BOX_X, BOX_Y, BOX_Z, TILE), 1.0, 6.0, ((1, 4), (2, 4), (3, 2)), jnp.float32)
    history = draw_history(jax.random.fold_in(key_of[6], 71), 0)
    return {"fractions": fractions, "polarizability": polarizability, "occupancy": occupancy, "pair_mask": pair_mask, "perm_field": perm_field, "history": history}


CELL_EDGE = 10.0
SOFTENING = 0.3
THOLE_DAMP = 0.39
RELAXATION = 0.7

def pair_field(target, source, moment, offset_vec, itself, allowed):
    displace = [(offset_vec[axis_num] + source[axis_num][:, None, :] - target[axis_num][:, :, None]) * CELL_EDGE for axis_num in range(3)]
    dist_sq = displace[0] * displace[0] + displace[1] * displace[1] + displace[2] * displace[2] + SOFTENING
    inv_cube = lax.rsqrt(dist_sq) / dist_sq
    thole_arg = dist_sq * jnp.sqrt(dist_sq) * lax.rsqrt(target[3][:, :, None] * source[3][:, None, :])
    damping = jnp.exp(-THOLE_DAMP * thole_arg)
    lambda_three = 1.0 - damping
    lambda_five = 1.0 - (1.0 + THOLE_DAMP * thole_arg) * damping
    slots = target.shape[-1]
    self_pair = jnp.logical_and(itself, jnp.eye(slots, dtype=bool))
    weight = jnp.where(self_pair, 0.0, allowed[:, None, None])
    radial = 3.0 * lambda_five * inv_cube / dist_sq * weight
    direct = lambda_three * inv_cube * weight
    fields = []
    for which_set in range(moment.shape[0] // 3):
        parts = [moment[3 * which_set + axis_num][:, None, :] for axis_num in range(3)]
        project = displace[0] * parts[0] + displace[1] * parts[1] + displace[2] * parts[2]
        for axis_num in range(3):
            fields.append(lax.optimization_barrier(jnp.sum(radial * project * displace[axis_num] - direct * parts[axis_num], axis=-1)))
    return jnp.stack(fields)

def slab_field(geometry_pad, moment_pad, allowed_slab, slab_index):
    width_y = geometry_pad.shape[2] - 2
    width_z = geometry_pad.shape[3] - 2
    slots = geometry_pad.shape[4]
    rows = moment_pad.shape[0]
    zero = jnp.zeros((), jnp.int32)
    one = jnp.ones((), jnp.int32)
    first_x = (jnp.asarray(slab_index) + 1).astype(jnp.int32)
    target = lax.dynamic_slice(geometry_pad, (zero, first_x, one, one, zero), (4, 1, width_y, width_z, slots)).reshape(4, width_y * width_z, slots)

    def offset_step(offset, summed):
        offset = jnp.asarray(offset).astype(jnp.int32)
        along_x = offset // 9 - 1
        along_y = offset // 3 % 3 - 1
        along_z = offset % 3 - 1
        starts = (zero, first_x + along_x, one + along_y, one + along_z, zero)
        source = lax.dynamic_slice(geometry_pad, starts, (4, 1, width_y, width_z, slots)).reshape(4, width_y * width_z, slots)
        moment = lax.dynamic_slice(moment_pad, starts, (rows, 1, width_y, width_z, slots)).reshape(rows, width_y * width_z, slots)
        allowed = lax.dynamic_index_in_dim(allowed_slab, offset, 2, keepdims=False).reshape(-1).astype(jnp.float32)
        offset_vec = jnp.stack([along_x, along_y, along_z]).astype(jnp.float32)
        return summed + pair_field(target, source, moment, offset_vec, offset == 13, allowed)
    summed = lax.fori_loop(0, 27, offset_step, jnp.zeros((rows, width_y * width_z, slots), jnp.float32))
    return summed.reshape(rows, width_y, width_z, slots)

def wrap_pad(values):
    return jnp.pad(values, ((0, 0), (1, 1), (1, 1), (1, 1), (0, 0)), mode='wrap')

def box_field(geometry_pad, moment, pair_mask):
    moment_pad = wrap_pad(moment)

    def one_slab(slab_index):
        allowed_slab = lax.dynamic_index_in_dim(pair_mask, slab_index, 0, keepdims=False)
        return slab_field(geometry_pad, moment_pad, allowed_slab, slab_index)
    slabs = lax.map(one_slab, jnp.arange(pair_mask.shape[0], dtype=jnp.int32))
    return jnp.moveaxis(slabs, 0, 1)

def fit_coefficients(gram_matrix):
    past_count = gram_matrix.shape[0] - 1
    gram_past = gram_matrix[:past_count, :past_count]
    gram_next = gram_matrix[:past_count, past_count]
    ridge_term = 0.001 * jnp.trace(gram_past) / past_count + 1.0
    factor = jnp.linalg.cholesky(gram_past + ridge_term * jnp.eye(past_count, dtype=jnp.float32))
    return jax.scipy.linalg.cho_solve((factor, True), gram_next)

def reference(fractions, polarizability, occupancy, pair_mask, perm_field, history):
    filled = occupancy.astype(jnp.float32)
    geometry = jnp.concatenate([fractions, polarizability[None]], 0)
    masked = history * filled
    flat_hist = masked.reshape(masked.shape[0], -1)
    gram_matrix = jnp.dot(flat_hist, flat_hist.T, precision=lax.Precision.HIGHEST)
    coeffs = fit_coefficients(gram_matrix)
    predicted = jnp.tensordot(coeffs, masked[1:], axes=1, precision=lax.Precision.HIGHEST)
    geometry_pad = wrap_pad(geometry)
    scaled = RELAXATION * filled * polarizability
    field_one = box_field(geometry_pad, predicted, pair_mask)
    dipole_one = (1.0 - RELAXATION) * predicted + scaled * (perm_field + field_one)
    field_two = box_field(geometry_pad, dipole_one, pair_mask)
    induced = (1.0 - RELAXATION) * dipole_one + scaled * (perm_field + field_two)
    update = induced - dipole_one
    change = jnp.sqrt(jnp.sum(update * update) / (jnp.sum(induced * induced) + 1.0))
    return (induced, change)
```

```python
import functools

import jax
import jax.numpy as jnp
from jax import lax
from jax.experimental import pallas as pl
from jax.experimental.pallas import tpu as pltpu
from jax.sharding import PartitionSpec as P

CELL_EDGE = 10.0
SOFTENING = 0.3
THOLE_DAMP = 0.39
RELAXATION = 0.7
MESH = pl.DeviceIdType.MESH
AXES = ("gx", "gy", "gz")
ROWS = 8
BLOCK = 32


def halo_moves(devices, tiles):
    options = []
    for count, n in zip(devices, tiles):
        if count == 2 and n == 2:
            around = [(1, 0, 2, 2)]
        else:
            around = [(1, n - 1, 1, n + 1), (-1, 0, 1, n)]
        options.append([(0, 0, n, 0)] + around)
    return [
        (a, b, c) for a in options[0] for b in options[1] for c in options[2] if (a[0], b[0], c[0]) != (0, 0, 0)
    ]


def solve_fit(total, past, lane, pair_lane):
    def pick(a, b):
        index = pair_lane[(min(a, b), max(a, b))]
        return jnp.sum(jnp.where(lane == index, total, 0.0), axis=1, keepdims=True)

    diagonal = [pick(a, a) for a in range(past)]
    trace = diagonal[0]
    for value in diagonal[1:]:
        trace = trace + value
    ridge = 0.001 * trace / past + 1.0
    lower, inverse = {}, []
    for j in range(past):
        pivot = diagonal[j] + ridge
        for m in range(j):
            pivot = pivot - lower[j, m] * lower[j, m]
        inverse.append(1.0 / jnp.sqrt(pivot))
        for i in range(j + 1, past):
            value = pick(i, j)
            for m in range(j):
                value = value - lower[i, m] * lower[j, m]
            lower[i, j] = value * inverse[j]
    forward = []
    for i in range(past):
        value = pick(i, past)
        for m in range(i):
            value = value - lower[i, m] * forward[m]
        forward.append(value * inverse[i])
    coeffs = [None] * past
    for i in reversed(range(past)):
        value = forward[i]
        for m in range(i + 1, past):
            value = value - lower[m, i] * coeffs[m]
        coeffs[i] = value * inverse[i]
    return coeffs


def kernel(
    devices,
    frac_ref, pol_ref, occ_ref, mask_ref, perm_ref, hist_ref,
    out_ref, change_ref,
    geom, held_one, held_two, past_sets, own, radial, direct, sums, slots_a, slots_b,
    send_all, recv_all, send_geom, recv_geom, send_one, recv_one, send_two, recv_two,
):
    tiles = tuple(frac_ref.shape[1:4])
    slots = frac_ref.shape[4]
    steps = hist_ref.shape[0]
    rows = hist_ref.shape[1]
    past = steps - 1
    total_devices = devices[0] * devices[1] * devices[2]
    at = [lax.axis_index(axis) for axis in AXES]
    me = (at[0] * devices[1] + at[1]) * devices[2] + at[2]
    moves = halo_moves(devices, tiles)
    lane = lax.broadcasted_iota(jnp.int32, (1, slots), 1)

    def coords(index):
        return (index // (devices[1] * devices[2]), index // devices[2] % devices[1], index % devices[2])

    barrier = pltpu.get_barrier_semaphore()

    def greet(step, carry):
        pl.semaphore_signal(
            barrier, inc=1, device_id=coords((me + step) % total_devices), device_id_type=MESH
        )
        return carry

    lax.fori_loop(1, total_devices, greet, 0)

    def everyone(index, held):
        def one(step):
            return pltpu.make_async_remote_copy(
                src_ref=held.at[pl.ds(me, 1)],
                dst_ref=held.at[pl.ds(me, 1)],
                send_sem=send_all.at[index],
                recv_sem=recv_all.at[index],
                device_id=coords((me + step) % total_devices),
                device_id_type=MESH,
            )

        def start(step, carry):
            one(step).start()
            return carry

        lax.fori_loop(1, total_devices, start, 0)

    def everyone_wait(index, held):
        whole = pltpu.make_async_remote_copy(
            src_ref=held.at[pl.ds(0, total_devices - 1)],
            dst_ref=held.at[pl.ds(0, total_devices - 1)],
            send_sem=send_all.at[index],
            recv_sem=recv_all.at[index],
            device_id=coords((me + 1) % total_devices),
            device_id_type=MESH,
        )
        whole.wait_send()
        whole.wait_recv()

    def halo(held, send, recv):
        copies = []
        for number, move in enumerate(moves):
            source = tuple(pl.ds(part[1], part[2]) for part in move)
            place = tuple(pl.ds(part[3], part[2]) for part in move)
            target = tuple((at[axis] + move[axis][0] + devices[axis]) % devices[axis] for axis in range(3))
            copies.append(
                pltpu.make_async_remote_copy(
                    src_ref=held.at[source],
                    dst_ref=held.at[place],
                    send_sem=send.at[number],
                    recv_sem=recv.at[number],
                    device_id=target,
                    device_id_type=MESH,
                )
            )
        return copies

    places = [(x, y, z) for x in range(tiles[0]) for y in range(tiles[1]) for z in range(tiles[2])]
    zero_row = jnp.zeros((1, slots), jnp.float32)
    spare = jnp.zeros((ROWS - rows, slots), jnp.float32)
    filled, scaled, fixed = [], [], []
    for t, (x, y, z) in enumerate(places):
        full = occ_ref[x, y, z, :].reshape(1, slots).astype(jnp.float32)
        pol = pol_ref[x, y, z, :].reshape(1, slots)
        scaled.append(RELAXATION * full * pol)
        tile = jnp.concatenate(
            [frac_ref[c, x, y, z, :].reshape(1, slots) * CELL_EDGE for c in range(3)]
            + [lax.rsqrt(pol)] + [zero_row] * (ROWS - 4),
            axis=0,
        )
        geom[x, y, z] = tile
        for h in range(steps):
            moment = jnp.concatenate(
                [hist_ref[h, c, x, y, z, :].reshape(1, slots) for c in range(rows)], axis=0
            )
            past_sets[h, t] = jnp.concatenate([moment * full, spare], axis=0)
        fixed.append(
            jnp.concatenate(
                [perm_ref[c, x, y, z, :].reshape(1, slots) for c in range(rows)] + [spare], axis=0
            )
        )
    pair_lane = {}
    gram = zero_row
    for a in range(steps):
        for b in range(a, steps):
            product = past_sets[a, 0] * past_sets[b, 0]
            for t in range(1, len(places)):
                product = product + past_sets[a, t] * past_sets[b, t]
            value = jnp.sum(jnp.sum(product, axis=0, keepdims=True), axis=1, keepdims=True)
            pair_lane[(a, b)] = len(pair_lane)
            gram = jnp.where(lane == pair_lane[(a, b)], value, gram)
    slots_a[pl.ds(me, 1)] = gram.reshape(1, 1, slots)

    pl.semaphore_wait(barrier, total_devices - 1)
    geom_copies = halo(geom, send_geom, recv_geom)
    everyone(0, slots_a)
    for copy in geom_copies:
        copy.start()

    for t, (x, y, z) in enumerate(places):
        for c in range(4):
            row = geom[x, y, z, c, :].reshape(1, slots)
            own[t, c] = jnp.broadcast_to(row, (slots, slots)).T

    everyone_wait(0, slots_a)
    total = jnp.sum(slots_a[...], axis=0)
    coeffs = solve_fit(total, past, lane, pair_lane)
    for t, (x, y, z) in enumerate(places):
        value = coeffs[0] * past_sets[1, t]
        for h in range(1, past):
            value = value + coeffs[h] * past_sets[h + 1, t]
        held_one[x, y, z] = value
    one_copies = halo(held_one, send_one, recv_one)
    for copy in one_copies:
        copy.start()
    for copy in geom_copies:
        copy.wait()

    wraps = tuple(n + 2 for n in tiles)

    def wrap(value, size):
        return jnp.where(value < 0, value + size, value)

    def spot(t, along):
        x = t // (tiles[1] * tiles[2])
        y = t // tiles[2] % tiles[1]
        z = t % tiles[2]
        return (x, y, z)

    def source_rows(held, place, names):
        return [held[place[0], place[1], place[2], pl.ds(c, 1), :] for c in names]

    def geometry(step, carry):
        t, k = step // 27, step % 27
        along = (k // 9 - 1, k // 3 % 3 - 1, k % 3 - 1)
        base = spot(t, along)
        place = tuple(wrap(base[i] + along[i], wraps[i]) for i in range(3))
        source = source_rows(geom, place, range(4))
        for i in range(3):
            source[i] = source[i] + CELL_EDGE * along[i].astype(jnp.float32)
        damp = source[3] * THOLE_DAMP
        allowed = mask_ref[base[0], base[1], base[2], k].astype(jnp.float32)
        for first in range(0, slots, BLOCK):
            part = pl.ds(first, BLOCK)
            dx = source[0] - own[t, 0, part, :]
            dy = source[1] - own[t, 1, part, :]
            dz = source[2] - own[t, 2, part, :]
            square = dx * dx + dy * dy + dz * dz + SOFTENING
            root = lax.rsqrt(square)
            root_two = root * root
            cube = root_two * root * allowed
            arg = (square * square) * root * (damp * own[t, 3, part, :])
            fade = jnp.exp(-arg)
            three = 1.0 - fade
            five = three - arg * fade
            direct[t, k, part, :] = three * cube
            radial[t, k, part, :] = five * cube * (3.0 * root_two)
        return carry

    count = len(places)
    lax.fori_loop(0, count * 27, geometry, 0)
    off_diagonal = lax.broadcasted_iota(jnp.int32, (slots, slots), 0) != lax.broadcasted_iota(
        jnp.int32, (slots, slots), 1
    )
    for t in range(count):
        direct[t, 13] = jnp.where(off_diagonal, direct[t, 13], 0.0)
        radial[t, 13] = jnp.where(off_diagonal, radial[t, 13], 0.0)

    ones = jnp.ones((ROWS, slots), jnp.float32)
    blocks = slots // BLOCK

    def field(held):
        def block_step(step, carry):
            t, part_index = step // blocks, step % blocks
            part = pl.ds(pl.multiple_of(part_index * BLOCK, BLOCK), BLOCK)
            base = spot(t, None)
            target = [own[t, c, part, :] for c in range(3)]

            def offsets(nine, acc):
                along_x, along_y = nine // 3 - 1, nine % 3 - 1
                acc = list(acc)
                for along_z in (-1, 0, 1):
                    along = (along_x, along_y, along_z)
                    place = tuple(wrap(base[i] + along[i], wraps[i]) for i in range(3))
                    source = source_rows(geom, place, range(3))
                    moment = source_rows(held, place, range(rows))
                    k = nine * 3 + along_z + 1
                    r = radial[t, k, part, :]
                    d = direct[t, k, part, :]
                    shift = [
                        CELL_EDGE * along_x.astype(jnp.float32),
                        CELL_EDGE * along_y.astype(jnp.float32),
                        CELL_EDGE * along_z,
                    ]
                    apart = [(source[i] + shift[i]) - target[i] for i in range(3)]
                    for s in range(rows // 3):
                        m = moment[3 * s : 3 * s + 3]
                        project = (apart[0] * m[0] + apart[1] * m[1] + apart[2] * m[2]) * r
                        for i in range(3):
                            acc[3 * s + i] = acc[3 * s + i] + (project * apart[i] - d * m[i])
                return tuple(acc)

            acc = lax.fori_loop(
                0, 9, offsets, tuple(jnp.zeros((BLOCK, slots), jnp.float32) for _ in range(rows))
            )
            for c in range(rows):
                sums[t, c, part, :] = acc[c]
            return carry

        lax.fori_loop(0, count * blocks, block_step, 0)
        fields = []
        for t in range(count):
            parts = [
                lax.dot_general(
                    ones, sums[t, c], (((1,), (1,)), ((), ())),
                    precision=lax.Precision.HIGHEST, preferred_element_type=jnp.float32,
                )[0:1]
                for c in range(rows)
            ]
            fields.append(jnp.concatenate(parts + [spare], axis=0))
        return fields

    for copy in one_copies:
        copy.wait()
    fields = field(held_one)
    for t, (x, y, z) in enumerate(places):
        held_two[x, y, z] = (1.0 - RELAXATION) * held_one[x, y, z] + scaled[t] * (fixed[t] + fields[t])
    two_copies = halo(held_two, send_two, recv_two)
    for copy in two_copies:
        copy.start()
    for copy in two_copies:
        copy.wait()
    fields = field(held_two)
    changed = jnp.zeros((ROWS, slots), jnp.float32)
    size = jnp.zeros((ROWS, slots), jnp.float32)
    for t, (x, y, z) in enumerate(places):
        before = held_two[x, y, z]
        after = (1.0 - RELAXATION) * before + scaled[t] * (fixed[t] + fields[t])
        for c in range(rows):
            out_ref[c, x, y, z, :] = after[c]
        changed = changed + (after - before) * (after - before)
        size = size + after * after

    def all_of(value):
        return jnp.sum(jnp.sum(value, axis=0, keepdims=True), axis=1, keepdims=True)

    pair = jnp.where(lane == 0, all_of(changed), jnp.where(lane == 1, all_of(size), 0.0))
    slots_b[pl.ds(me, 1)] = pair.reshape(1, 1, slots)
    everyone(1, slots_b)
    everyone_wait(1, slots_b)
    pair = jnp.sum(slots_b[...], axis=0)
    above = jnp.sum(jnp.where(lane == 0, pair, 0.0), axis=1, keepdims=True)
    below = jnp.sum(jnp.where(lane == 1, pair, 0.0), axis=1, keepdims=True)
    change_ref[...] = jnp.broadcast_to(jnp.sqrt(above / (below + 1.0)), (1, slots))


def solution(mesh):
    devices = tuple(mesh.shape[axis] for axis in AXES)
    total_devices = devices[0] * devices[1] * devices[2]

    def on_device(fractions, polarizability, occupancy, pair_mask, perm_field, history):
        tiles = fractions.shape[1:4]
        slots = fractions.shape[4]
        count = tiles[0] * tiles[1] * tiles[2]
        wraps = tuple(n + 2 for n in tiles)
        moves = len(halo_moves(devices, tiles))
        rows = history.shape[1]
        vmem = pl.BlockSpec(memory_space=pltpu.VMEM)
        smem = pl.BlockSpec(memory_space=pltpu.SMEM)
        f32 = jnp.float32
        induced, change = pl.pallas_call(
            functools.partial(kernel, devices),
            out_shape=(
                jax.ShapeDtypeStruct(perm_field.shape, f32),
                jax.ShapeDtypeStruct((1, slots), f32),
            ),
            in_specs=[vmem, vmem, vmem, smem, vmem, vmem],
            out_specs=(vmem, vmem),
            scratch_shapes=[
                pltpu.VMEM(wraps + (ROWS, slots), f32),
                pltpu.VMEM(wraps + (ROWS, slots), f32),
                pltpu.VMEM(wraps + (ROWS, slots), f32),
                pltpu.VMEM((history.shape[0], count, ROWS, slots), f32),
                pltpu.VMEM((count, 4, slots, slots), f32),
                pltpu.VMEM((count, 27, slots, slots), f32),
                pltpu.VMEM((count, 27, slots, slots), f32),
                pltpu.VMEM((count, rows, slots, slots), f32),
                pltpu.VMEM((total_devices, 1, slots), f32),
                pltpu.VMEM((total_devices, 1, slots), f32),
                pltpu.SemaphoreType.DMA((2,)),
                pltpu.SemaphoreType.DMA((2,)),
            ]
            + [pltpu.SemaphoreType.DMA((moves,))] * 6,
            compiler_params=pltpu.CompilerParams(
                collective_id=0, has_side_effects=True, vmem_limit_bytes=40 * 1024 * 1024
            ),
        )(fractions, polarizability, occupancy, pair_mask, perm_field, history)
        return induced, change[0, 0]

    in_specs = (
        P(None, "gx", "gy", "gz", None),
        P("gx", "gy", "gz", None),
        P("gx", "gy", "gz", None),
        P("gx", "gy", "gz", None),
        P(None, "gx", "gy", "gz", None),
        P(None, None, "gx", "gy", "gz", None),
    )
    out_specs = (P(None, "gx", "gy", "gz", None), P())
    return jax.shard_map(
        on_device, mesh=mesh, in_specs=in_specs, out_specs=out_specs, check_vma=False
    )
```

```python
import functools

import jax
import jax.numpy as jnp
from jax import lax
from jax.experimental import pallas as pl
from jax.experimental.pallas import tpu as pltpu
from jax.sharding import PartitionSpec as P

CELL_EDGE = 10.0
SOFTENING = 0.3
THOLE_DAMP = 0.39
RELAXATION = 0.7
MESH = pl.DeviceIdType.MESH
AXES = ("gx", "gy", "gz")
ROWS = 8
BLOCK = 32
FIELD_BLOCK = 32


def halo_moves(devices, tiles):
    options = []
    for count, n in zip(devices, tiles):
        if count == 2 and n == 2:
            around = [(1, 0, 2, 2)]
        else:
            around = [(1, n - 1, 1, n + 1), (-1, 0, 1, n)]
        options.append([(0, 0, n, 0)] + around)
    return [
        (a, b, c) for a in options[0] for b in options[1] for c in options[2] if (a[0], b[0], c[0]) != (0, 0, 0)
    ]


def row_moves(devices, tiles, row):
    along_x, along_y, along_z = [
        [(0, 0, n, 0)] + [move[axis] for move in halo_moves(devices, tiles) if move[axis][0] != 0]
        for axis, n in enumerate(tiles)
    ]
    n = tiles[1]
    rows = [(0, row, 1, row)]
    if row == n - 1:
        rows.append((1, row, 1, n + 1))
    if row == 0:
        rows.append((-1, row, 1, n))
    along_x, along_z = list(dict.fromkeys(along_x)), list(dict.fromkeys(along_z))
    return [
        (a, b, c) for a in along_x for b in rows for c in along_z if (a[0], b[0], c[0]) != (0, 0, 0)
    ]


def solve_fit(total, past, lane, pair_lane):
    def pick(a, b):
        index = pair_lane[(min(a, b), max(a, b))]
        return jnp.sum(jnp.where(lane == index, total, 0.0), axis=1, keepdims=True)

    diagonal = [pick(a, a) for a in range(past)]
    trace = diagonal[0]
    for value in diagonal[1:]:
        trace = trace + value
    ridge = 0.001 * trace / past + 1.0
    lower, inverse = {}, []
    for j in range(past):
        pivot = diagonal[j] + ridge
        for m in range(j):
            pivot = pivot - lower[j, m] * lower[j, m]
        inverse.append(1.0 / jnp.sqrt(pivot))
        for i in range(j + 1, past):
            value = pick(i, j)
            for m in range(j):
                value = value - lower[i, m] * lower[j, m]
            lower[i, j] = value * inverse[j]
    forward = []
    for i in range(past):
        value = pick(i, past)
        for m in range(i):
            value = value - lower[i, m] * forward[m]
        forward.append(value * inverse[i])
    coeffs = [None] * past
    for i in reversed(range(past)):
        value = forward[i]
        for m in range(i + 1, past):
            value = value - lower[m, i] * coeffs[m]
        coeffs[i] = value * inverse[i]
    return coeffs


def kernel(
    devices,
    frac_in, pol_in, occ_in, mask_in, perm_in, hist_in,
    out_ref, change_ref,
    frac_ref, pol_ref, occ_ref, mask_ref, perm_ref, hist_ref,
    geom, held_one, held_two, past_sets, own, radial, direct, sums, slots_a, slots_b,
    load_sem, send_all, recv_all, send_geom, recv_geom, send_one, recv_one, send_two, recv_two,
):
    tiles = tuple(frac_ref.shape[1:4])
    slots = frac_ref.shape[4]
    steps = hist_ref.shape[0]
    rows = hist_ref.shape[1]
    past = steps - 1
    total_devices = devices[0] * devices[1] * devices[2]
    at = [lax.axis_index(axis) for axis in AXES]
    me = (at[0] * devices[1] + at[1]) * devices[2] + at[2]
    moves = halo_moves(devices, tiles)
    lane = lax.broadcasted_iota(jnp.int32, (1, slots), 1)
    loads = [
        pltpu.make_async_copy(source, target, load_sem.at[number])
        for number, (source, target) in enumerate(
            (
                (hist_in, hist_ref), (occ_in, occ_ref), (frac_in, frac_ref),
                (pol_in, pol_ref), (perm_in, perm_ref), (mask_in, mask_ref),
            )
        )
    ]
    for load in loads:
        load.start()

    def coords(index):
        return (index // (devices[1] * devices[2]), index // devices[2] % devices[1], index % devices[2])

    barrier = pltpu.get_barrier_semaphore()

    def greet(step, carry):
        pl.semaphore_signal(
            barrier, inc=1, device_id=coords((me + step) % total_devices), device_id_type=MESH
        )
        return carry

    lax.fori_loop(1, total_devices, greet, 0)
    for load in loads:
        load.wait()

    def everyone(index, held):
        def one(step):
            return pltpu.make_async_remote_copy(
                src_ref=held.at[pl.ds(me, 1)],
                dst_ref=held.at[pl.ds(me, 1)],
                send_sem=send_all.at[index],
                recv_sem=recv_all.at[index],
                device_id=coords((me + step) % total_devices),
                device_id_type=MESH,
            )

        def start(step, carry):
            one(step).start()
            return carry

        lax.fori_loop(1, total_devices, start, 0)

    def everyone_wait(index, held):
        whole = pltpu.make_async_remote_copy(
            src_ref=held.at[pl.ds(0, total_devices - 1)],
            dst_ref=held.at[pl.ds(0, total_devices - 1)],
            send_sem=send_all.at[index],
            recv_sem=recv_all.at[index],
            device_id=coords((me + 1) % total_devices),
            device_id_type=MESH,
        )
        whole.wait_send()
        whole.wait_recv()

    def halo(held, send, recv, moves=moves):
        copies = []
        for number, move in enumerate(moves):
            source = tuple(pl.ds(part[1], part[2]) for part in move)
            place = tuple(pl.ds(part[3], part[2]) for part in move)
            target = tuple((at[axis] + move[axis][0] + devices[axis]) % devices[axis] for axis in range(3))
            copies.append(
                pltpu.make_async_remote_copy(
                    src_ref=held.at[source],
                    dst_ref=held.at[place],
                    send_sem=send.at[number],
                    recv_sem=recv.at[number],
                    device_id=target,
                    device_id_type=MESH,
                )
            )
        return copies

    places = [(x, y, z) for x in range(tiles[0]) for y in range(tiles[1]) for z in range(tiles[2])]
    zero_row = jnp.zeros((1, slots), jnp.float32)
    spare = jnp.zeros((ROWS - rows, slots), jnp.float32)
    filled, scaled, fixed = [], [], []
    for t, (x, y, z) in enumerate(places):
        full = occ_ref[x, y, z, :].reshape(1, slots).astype(jnp.float32)
        pol = pol_ref[x, y, z, :].reshape(1, slots)
        scaled.append(RELAXATION * full * pol)
        tile = jnp.concatenate(
            [frac_ref[c, x, y, z, :].reshape(1, slots) * CELL_EDGE for c in range(3)]
            + [lax.rsqrt(pol)] + [zero_row] * (ROWS - 4),
            axis=0,
        )
        geom[x, y, z] = tile
        for h in range(steps):
            moment = jnp.concatenate(
                [hist_ref[h, c, x, y, z, :].reshape(1, slots) for c in range(rows)], axis=0
            )
            past_sets[h, t] = jnp.concatenate([moment * full, spare], axis=0)
        fixed.append(
            jnp.concatenate(
                [perm_ref[c, x, y, z, :].reshape(1, slots) for c in range(rows)] + [spare], axis=0
            )
        )
    pair_lane = {}
    gram = zero_row
    for a in range(steps):
        for b in range(a, steps):
            product = past_sets[a, 0] * past_sets[b, 0]
            for t in range(1, len(places)):
                product = product + past_sets[a, t] * past_sets[b, t]
            value = jnp.sum(jnp.sum(product, axis=0, keepdims=True), axis=1, keepdims=True)
            pair_lane[(a, b)] = len(pair_lane)
            gram = jnp.where(lane == pair_lane[(a, b)], value, gram)
    slots_a[pl.ds(me, 1)] = gram.reshape(1, 1, slots)

    for t, (x, y, z) in enumerate(places):
        for c in range(4):
            row = geom[x, y, z, c, :].reshape(1, slots)
            own[t, c] = jnp.broadcast_to(row, (slots, slots)).T

    pl.semaphore_wait(barrier, total_devices - 1)
    geom_copies = halo(geom, send_geom, recv_geom)
    everyone(0, slots_a)
    for copy in geom_copies:
        copy.start()

    def clear(step, carry):
        sums[step] = jnp.zeros((rows, slots, slots), jnp.float32)
        return carry

    lax.fori_loop(0, 2 * len(places), clear, 0)
    for copy in geom_copies:
        copy.wait()

    wraps = tuple(n + 2 for n in tiles)

    def wrap(value, size):
        return jnp.where(value < 0, value + size, value)

    def spot(t):
        x = t // (tiles[1] * tiles[2])
        y = t // tiles[2] % tiles[1]
        z = t % tiles[2]
        return (x, y, z)

    def source_rows(held, place, names):
        return [held[place[0], place[1], place[2], pl.ds(c, 1), :] for c in names]

    def geometry(step, carry):
        t, nine = step // 9, step % 9
        along_x, along_y = nine // 3 - 1, nine % 3 - 1
        base = spot(t)
        for along_z in (-1, 0, 1):
            along = (along_x, along_y, along_z)
            k = nine * 3 + along_z + 1
            place = tuple(wrap(base[i] + along[i], wraps[i]) for i in range(3))
            source = source_rows(geom, place, range(4))
            source[0] = source[0] + CELL_EDGE * along_x.astype(jnp.float32)
            source[1] = source[1] + CELL_EDGE * along_y.astype(jnp.float32)
            source[2] = source[2] + CELL_EDGE * along_z
            damp = source[3] * THOLE_DAMP
            allowed = mask_ref[base[0], base[1], base[2], k].astype(jnp.float32)
            for first in range(0, slots, BLOCK):
                part = pl.ds(first, BLOCK)
                dx = source[0] - own[t, 0, part, :]
                dy = source[1] - own[t, 1, part, :]
                dz = source[2] - own[t, 2, part, :]
                square = dx * dx + dy * dy + dz * dz + SOFTENING
                root = lax.rsqrt(square)
                root_two = root * root
                cube = root_two * root * allowed
                arg = (square * square) * root * (damp * own[t, 3, part, :])
                fade = jnp.exp(-arg)
                three = 1.0 - fade
                five = three - arg * fade
                direct[t, k, part, :] = three * cube
                radial[t, k, part, :] = five * cube * (3.0 * root_two)
        return carry

    count = len(places)
    early = count * 9 // 3
    lax.fori_loop(0, early, geometry, 0)

    everyone_wait(0, slots_a)
    total = jnp.sum(slots_a[...], axis=0)
    coeffs = solve_fit(total, past, lane, pair_lane)
    for t, (x, y, z) in enumerate(places):
        value = coeffs[0] * past_sets[1, t]
        for h in range(1, past):
            value = value + coeffs[h] * past_sets[h + 1, t]
        held_one[x, y, z] = value
    one_copies = halo(held_one, send_one, recv_one)
    for copy in one_copies:
        copy.start()
    lax.fori_loop(early, count * 9, geometry, 0)
    off_diagonal = lax.broadcasted_iota(jnp.int32, (slots, slots), 0) != lax.broadcasted_iota(
        jnp.int32, (slots, slots), 1
    )
    for t in range(count):
        direct[t, 13] = jnp.where(off_diagonal, direct[t, 13], 0.0)
        radial[t, 13] = jnp.where(off_diagonal, radial[t, 13], 0.0)

    blocks = slots // FIELD_BLOCK

    def add_sources(held, index, step, base, along_y):
        part = pl.ds(pl.multiple_of(step % blocks * FIELD_BLOCK, FIELD_BLOCK), FIELD_BLOCK)
        t = (base[0] * tiles[1] + base[1]) * tiles[2] + base[2]
        place_y = wrap(base[1] + along_y, wraps[1])
        target = [own[t, c, part, :] for c in range(3)]
        target[1] = target[1] - CELL_EDGE * along_y.astype(jnp.float32)
        deep = [target[2] - CELL_EDGE * along_z for along_z in (-1, 0, 1)]

        def plane(along_x, acc):
            acc = list(acc)
            place_x = wrap(base[0] + along_x, wraps[0])
            wide = target[0] - CELL_EDGE * along_x
            for along_z in (-1, 0, 1):
                place = (place_x, place_y, wrap(base[2] + along_z, wraps[2]))
                source = source_rows(geom, place, range(3))
                moment = source_rows(held, place, range(rows))
                k = 9 * (along_x + 1) + 3 * (along_y + 1) + along_z + 1
                r = radial[t, k, part, :]
                d = direct[t, k, part, :]
                apart = [source[0] - wide, source[1] - target[1], source[2] - deep[along_z + 1]]
                for s in range(rows // 3):
                    m = moment[3 * s : 3 * s + 3]
                    project = (apart[0] * m[0] + apart[1] * m[1] + apart[2] * m[2]) * r
                    for i in range(3):
                        acc[3 * s + i] = acc[3 * s + i] + (project * apart[i] - d * m[i])
            return tuple(acc)

        acc = tuple(sums[index * count + t, c, part, :] for c in range(rows))
        for along_x in (-1, 0, 1):
            acc = plane(along_x, acc)
        for c in range(rows):
            sums[index * count + t, c, part, :] = acc[c]

    flat = tiles[0] * tiles[2] * blocks

    def to_row(held, index, row):
        def one(step, carry):
            column = step // blocks % (tiles[0] * tiles[2])
            base = (column // tiles[2], row, column % tiles[2])
            add_sources(held, index, step, base, step // flat - 1)
            return carry

        lax.fori_loop(0, 3 * flat, one, 0)

    def from_row(held, index, row):
        def one(step, carry):
            column = step // blocks % (tiles[0] * tiles[2])
            along_y = step // flat - 1
            base = (column // tiles[2], (row - along_y + tiles[1]) % tiles[1], column % tiles[2])
            add_sources(held, index, step, base, along_y)
            return carry

        lax.fori_loop(0, 3 * flat, one, 0)

    square_lane = lax.broadcasted_iota(jnp.int32, (slots, slots), 1)

    def field_of(index, t):
        columns = jnp.zeros((slots, slots), jnp.float32)
        for c in range(rows):
            value = jnp.sum(sums[index * count + t, c], axis=1, keepdims=True)
            columns = jnp.where(square_lane == c, value, columns)
        return columns.T[0:ROWS]

    for copy in one_copies:
        copy.wait()
    two_copies = []
    for row in range(tiles[1]):
        to_row(held_one, 0, row)
        for t, (x, y, z) in enumerate(places):
            if y == row:
                held_two[x, y, z] = (1.0 - RELAXATION) * held_one[x, y, z] + scaled[t] * (
                    fixed[t] + field_of(0, t)
                )
        copies = halo(held_two, send_two.at[row], recv_two.at[row], row_moves(devices, tiles, row))
        for copy in copies:
            copy.start()
        two_copies.append(copies)
    for row in range(tiles[1]):
        for copy in two_copies[row]:
            copy.wait()
        from_row(held_two, 1, row)
    fields = [field_of(1, t) for t in range(count)]
    changed = jnp.zeros((ROWS, slots), jnp.float32)
    size = jnp.zeros((ROWS, slots), jnp.float32)
    for t, (x, y, z) in enumerate(places):
        before = held_two[x, y, z]
        after = (1.0 - RELAXATION) * before + scaled[t] * (fixed[t] + fields[t])
        for c in range(rows):
            out_ref[c, x, y, z, :] = after[c]
        changed = changed + (after - before) * (after - before)
        size = size + after * after

    def all_of(value):
        return jnp.sum(jnp.sum(value, axis=0, keepdims=True), axis=1, keepdims=True)

    pair = jnp.where(lane == 0, all_of(changed), jnp.where(lane == 1, all_of(size), 0.0))
    slots_b[pl.ds(me, 1)] = pair.reshape(1, 1, slots)
    everyone(1, slots_b)
    everyone_wait(1, slots_b)
    pair = jnp.sum(slots_b[...], axis=0)
    above = jnp.sum(jnp.where(lane == 0, pair, 0.0), axis=1, keepdims=True)
    below = jnp.sum(jnp.where(lane == 1, pair, 0.0), axis=1, keepdims=True)
    change_ref[...] = jnp.broadcast_to(jnp.sqrt(above / (below + 1.0)), (1, slots))


def solution(mesh):
    devices = tuple(mesh.shape[axis] for axis in AXES)
    total_devices = devices[0] * devices[1] * devices[2]

    def on_device(fractions, polarizability, occupancy, pair_mask, perm_field, history):
        tiles = fractions.shape[1:4]
        slots = fractions.shape[4]
        count = tiles[0] * tiles[1] * tiles[2]
        wraps = tuple(n + 2 for n in tiles)
        moves = len(halo_moves(devices, tiles))
        rows = history.shape[1]
        vmem = pl.BlockSpec(memory_space=pltpu.VMEM)
        f32 = jnp.float32
        induced, change = pl.pallas_call(
            functools.partial(kernel, devices),
            out_shape=(
                jax.ShapeDtypeStruct(perm_field.shape, f32),
                jax.ShapeDtypeStruct((1, slots), f32),
            ),
            in_specs=[pl.BlockSpec(memory_space=pltpu.HBM)] * 6,
            out_specs=(vmem, vmem),
            scratch_shapes=[
                pltpu.VMEM(fractions.shape, f32),
                pltpu.VMEM(polarizability.shape, f32),
                pltpu.VMEM(occupancy.shape, jnp.int32),
                pltpu.SMEM(pair_mask.shape, jnp.int32),
                pltpu.VMEM(perm_field.shape, f32),
                pltpu.VMEM(history.shape, f32),
                pltpu.VMEM(wraps + (ROWS, slots), f32),
                pltpu.VMEM(wraps + (ROWS, slots), f32),
                pltpu.VMEM(wraps + (ROWS, slots), f32),
                pltpu.VMEM((history.shape[0], count, ROWS, slots), f32),
                pltpu.VMEM((count, 4, slots, slots), f32),
                pltpu.VMEM((count, 27, slots, slots), f32),
                pltpu.VMEM((count, 27, slots, slots), f32),
                pltpu.VMEM((2 * count, rows, slots, slots), f32),
                pltpu.VMEM((total_devices, 1, slots), f32),
                pltpu.VMEM((total_devices, 1, slots), f32),
                pltpu.SemaphoreType.DMA((6,)),
                pltpu.SemaphoreType.DMA((2,)),
                pltpu.SemaphoreType.DMA((2,)),
            ]
            + [pltpu.SemaphoreType.DMA((moves,))] * 4
            + [pltpu.SemaphoreType.DMA((tiles[1], moves))] * 2,
            compiler_params=pltpu.CompilerParams(
                collective_id=0, has_side_effects=True, vmem_limit_bytes=67043328
            ),
        )(fractions, polarizability, occupancy, pair_mask, perm_field, history)
        return induced, change[0, 0]

    in_specs = (
        P(None, "gx", "gy", "gz", None),
        P("gx", "gy", "gz", None),
        P("gx", "gy", "gz", None),
        P("gx", "gy", "gz", None),
        P(None, "gx", "gy", "gz", None),
        P(None, None, "gx", "gy", "gz", None),
    )
    out_specs = (P(None, "gx", "gy", "gz", None), P())
    return jax.shard_map(
        on_device, mesh=mesh, in_specs=in_specs, out_specs=out_specs, check_vma=False
    )
```

```python
import functools

import jax
import jax.numpy as jnp
from jax import lax
from jax.experimental import pallas as pl
from jax.experimental.pallas import tpu as pltpu
from jax.sharding import PartitionSpec as P

CELL_EDGE = 10.0
SOFTENING = 0.3
THOLE_DAMP = 0.39
RELAXATION = 0.7
MESH = pl.DeviceIdType.MESH
AXES = ("gx", "gy", "gz")
ROWS = 8
BLOCK = 32
FIELD_BLOCK = 32


def halo_moves(devices, tiles):
    options = []
    for count, n in zip(devices, tiles):
        if count == 2 and n == 2:
            around = [(1, 0, 2, 2)]
        else:
            around = [(1, n - 1, 1, n + 1), (-1, 0, 1, n)]
        options.append([(0, 0, n, 0)] + around)
    return [
        (a, b, c) for a in options[0] for b in options[1] for c in options[2] if (a[0], b[0], c[0]) != (0, 0, 0)
    ]


def row_moves(devices, tiles, row):
    along_x, along_y, along_z = [
        [(0, 0, n, 0)] + [move[axis] for move in halo_moves(devices, tiles) if move[axis][0] != 0]
        for axis, n in enumerate(tiles)
    ]
    n = tiles[1]
    rows = [(0, row, 1, row)]
    if row == n - 1:
        rows.append((1, row, 1, n + 1))
    if row == 0:
        rows.append((-1, row, 1, n))
    along_x, along_z = list(dict.fromkeys(along_x)), list(dict.fromkeys(along_z))
    return [
        (a, b, c) for a in along_x for b in rows for c in along_z if (a[0], b[0], c[0]) != (0, 0, 0)
    ]


def solve_fit(total, past, lane, pair_lane):
    def pick(a, b):
        index = pair_lane[(min(a, b), max(a, b))]
        return jnp.sum(jnp.where(lane == index, total, 0.0), axis=1, keepdims=True)

    diagonal = [pick(a, a) for a in range(past)]
    trace = diagonal[0]
    for value in diagonal[1:]:
        trace = trace + value
    ridge = 0.001 * trace / past + 1.0
    lower, inverse = {}, []
    for j in range(past):
        pivot = diagonal[j] + ridge
        for m in range(j):
            pivot = pivot - lower[j, m] * lower[j, m]
        inverse.append(1.0 / jnp.sqrt(pivot))
        for i in range(j + 1, past):
            value = pick(i, j)
            for m in range(j):
                value = value - lower[i, m] * lower[j, m]
            lower[i, j] = value * inverse[j]
    forward = []
    for i in range(past):
        value = pick(i, past)
        for m in range(i):
            value = value - lower[i, m] * forward[m]
        forward.append(value * inverse[i])
    coeffs = [None] * past
    for i in reversed(range(past)):
        value = forward[i]
        for m in range(i + 1, past):
            value = value - lower[m, i] * coeffs[m]
        coeffs[i] = value * inverse[i]
    return coeffs


def kernel(
    devices,
    frac_in, pol_in, occ_in, mask_in, perm_in, hist_in,
    out_ref, change_ref,
    frac_ref, pol_ref, occ_ref, mask_ref, perm_ref, hist_ref,
    geom, held_one, held_two, past_sets, own, apart, pull, direct, sums, slots_a, slots_b,
    load_sem, send_all, recv_all, send_geom, recv_geom, send_one, recv_one, send_two, recv_two,
):
    tiles = tuple(frac_ref.shape[1:4])
    slots = frac_ref.shape[4]
    steps = hist_ref.shape[0]
    rows = hist_ref.shape[1]
    past = steps - 1
    total_devices = devices[0] * devices[1] * devices[2]
    at = [lax.axis_index(axis) for axis in AXES]
    me = (at[0] * devices[1] + at[1]) * devices[2] + at[2]
    moves = halo_moves(devices, tiles)
    lane = lax.broadcasted_iota(jnp.int32, (1, slots), 1)
    loads = [
        pltpu.make_async_copy(source, target, load_sem.at[number])
        for number, (source, target) in enumerate(
            (
                (hist_in, hist_ref), (occ_in, occ_ref), (frac_in, frac_ref),
                (pol_in, pol_ref), (perm_in, perm_ref), (mask_in, mask_ref),
            )
        )
    ]
    for load in loads:
        load.start()

    def each_other(act):
        def pair(step, carry):
            ahead = (step // devices[1], step % devices[1])
            first = []
            for axis in range(2):
                place = at[axis] + ahead[axis]
                first.append(jnp.where(place >= devices[axis], place - devices[axis], place))
            for shift in range(devices[2] - 1, -1, -1):
                last = at[2] + shift
                last = jnp.where(last >= devices[2], last - devices[2], last)
                if shift == 0:
                    @pl.when(step > 0)
                    def _():
                        act((first[0], first[1], last))
                else:
                    act((first[0], first[1], last))
            return carry

        lax.fori_loop(0, devices[0] * devices[1], pair, 0)

    barrier = pltpu.get_barrier_semaphore()

    each_other(
        lambda device: pl.semaphore_signal(barrier, inc=1, device_id=device, device_id_type=MESH)
    )
    for load in loads:
        load.wait()

    def everyone(index, held):
        def start(device):
            pltpu.make_async_remote_copy(
                src_ref=held.at[pl.ds(me, 1)],
                dst_ref=held.at[pl.ds(me, 1)],
                send_sem=send_all.at[index],
                recv_sem=recv_all.at[index],
                device_id=device,
                device_id_type=MESH,
            ).start()

        each_other(start)

    def everyone_wait(index, held):
        whole = pltpu.make_async_remote_copy(
            src_ref=held.at[pl.ds(0, total_devices - 1)],
            dst_ref=held.at[pl.ds(0, total_devices - 1)],
            send_sem=send_all.at[index],
            recv_sem=recv_all.at[index],
            device_id=(at[0], at[1], (at[2] + 1) % devices[2]),
            device_id_type=MESH,
        )
        whole.wait_send()
        whole.wait_recv()

    def halo(held, send, recv, moves=moves):
        copies = []
        for number, move in enumerate(moves):
            source = tuple(pl.ds(part[1], part[2]) for part in move)
            place = tuple(pl.ds(part[3], part[2]) for part in move)
            target = tuple((at[axis] + move[axis][0] + devices[axis]) % devices[axis] for axis in range(3))
            copies.append(
                pltpu.make_async_remote_copy(
                    src_ref=held.at[source],
                    dst_ref=held.at[place],
                    send_sem=send.at[number],
                    recv_sem=recv.at[number],
                    device_id=target,
                    device_id_type=MESH,
                )
            )
        return copies

    places = [(x, y, z) for x in range(tiles[0]) for y in range(tiles[1]) for z in range(tiles[2])]
    zero_row = jnp.zeros((1, slots), jnp.float32)
    spare = jnp.zeros((ROWS - rows, slots), jnp.float32)
    filled, scaled, fixed = [], [], []
    for t, (x, y, z) in enumerate(places):
        full = occ_ref[x, y, z, :].reshape(1, slots).astype(jnp.float32)
        pol = pol_ref[x, y, z, :].reshape(1, slots)
        scaled.append(RELAXATION * full * pol)
        tile = jnp.concatenate(
            [frac_ref[c, x, y, z, :].reshape(1, slots) * CELL_EDGE for c in range(3)]
            + [lax.rsqrt(pol)] + [zero_row] * (ROWS - 4),
            axis=0,
        )
        geom[x, y, z] = tile
        for h in range(steps):
            moment = jnp.concatenate(
                [hist_ref[h, c, x, y, z, :].reshape(1, slots) for c in range(rows)], axis=0
            )
            past_sets[h, t] = jnp.concatenate([moment * full, spare], axis=0)
        fixed.append(
            jnp.concatenate(
                [perm_ref[c, x, y, z, :].reshape(1, slots) for c in range(rows)] + [spare], axis=0
            )
        )
    pair_lane = {}
    gram = zero_row
    for a in range(steps):
        for b in range(a, steps):
            product = past_sets[a, 0] * past_sets[b, 0]
            for t in range(1, len(places)):
                product = product + past_sets[a, t] * past_sets[b, t]
            value = jnp.sum(jnp.sum(product, axis=0, keepdims=True), axis=1, keepdims=True)
            pair_lane[(a, b)] = len(pair_lane)
            gram = jnp.where(lane == pair_lane[(a, b)], value, gram)
    slots_a[pl.ds(me, 1)] = gram.reshape(1, 1, slots)

    for t, (x, y, z) in enumerate(places):
        for c in range(4):
            row = geom[x, y, z, c, :].reshape(1, slots)
            own[t, c] = jnp.broadcast_to(row, (slots, slots)).T

    pl.semaphore_wait(barrier, total_devices - 1)
    geom_copies = halo(geom, send_geom, recv_geom)
    everyone(0, slots_a)
    for copy in geom_copies:
        copy.start()

    def clear(step, carry):
        sums[step] = jnp.zeros((rows, slots, slots), jnp.float32)
        return carry

    lax.fori_loop(0, 2 * len(places), clear, 0)
    for move, copy in zip(moves, geom_copies):
        if move[0][0] == 0:
            copy.wait()

    wraps = tuple(n + 2 for n in tiles)

    def wrap(value, size):
        return jnp.where(value < 0, value + size, value)

    def spot(t):
        x = t // (tiles[1] * tiles[2])
        y = t // tiles[2] % tiles[1]
        z = t % tiles[2]
        return (x, y, z)

    def source_rows(held, place, names):
        return [held[place[0], place[1], place[2], pl.ds(c, 1), :] for c in names]

    def geometry(t, nine):
        along_x, along_y = nine // 3 - 1, nine % 3 - 1
        base = spot(t)
        for along_z in (-1, 0, 1):
            along = (along_x, along_y, along_z)
            k = nine * 3 + along_z + 1
            place = tuple(wrap(base[i] + along[i], wraps[i]) for i in range(3))
            source = source_rows(geom, place, range(4))
            source[0] = source[0] + CELL_EDGE * along_x.astype(jnp.float32)
            source[1] = source[1] + CELL_EDGE * along_y.astype(jnp.float32)
            source[2] = source[2] + CELL_EDGE * along_z
            damp = source[3] * THOLE_DAMP
            allowed = mask_ref[base[0], base[1], base[2], k].astype(jnp.float32)
            for first in range(0, slots, BLOCK):
                part = pl.ds(first, BLOCK)
                dx = source[0] - own[t, 0, part, :]
                dy = source[1] - own[t, 1, part, :]
                dz = source[2] - own[t, 2, part, :]
                square = dx * dx + dy * dy + dz * dz + SOFTENING
                root = lax.rsqrt(square)
                root_two = root * root
                cube = root_two * root * allowed
                arg = (square * square) * root * (damp * own[t, 3, part, :])
                fade = jnp.exp(-arg)
                three = 1.0 - fade
                five = three - arg * fade
                direct[t, k, part, :] = three * cube
                radial = five * cube * (3.0 * root_two)
                for i, d in enumerate((dx, dy, dz)):
                    apart[i, t, k, part, :] = d
                    pull[i, t, k, part, :] = radial * d

    count = len(places)

    def same_x(step, carry):
        geometry(step // 3, 3 + step % 3)
        return carry

    def other_x(step, carry):
        part = step % 6
        geometry(step // 6, jnp.where(part < 3, part, part + 3))
        return carry

    lax.fori_loop(0, count * 3, same_x, 0)

    everyone_wait(0, slots_a)
    total = jnp.sum(slots_a[...], axis=0)
    coeffs = solve_fit(total, past, lane, pair_lane)
    for t, (x, y, z) in enumerate(places):
        value = coeffs[0] * past_sets[1, t]
        for h in range(1, past):
            value = value + coeffs[h] * past_sets[h + 1, t]
        held_one[x, y, z] = value
    one_copies = halo(held_one, send_one, recv_one)
    for copy in one_copies:
        copy.start()
    for move, copy in zip(moves, geom_copies):
        if move[0][0] != 0:
            copy.wait()
    lax.fori_loop(0, count * 6, other_x, 0)
    off_diagonal = lax.broadcasted_iota(jnp.int32, (slots, slots), 0) != lax.broadcasted_iota(
        jnp.int32, (slots, slots), 1
    )
    for t in range(count):
        direct[t, 13] = jnp.where(off_diagonal, direct[t, 13], 0.0)

    blocks = slots // FIELD_BLOCK

    def add_sources(held, index, step, base, along_y):
        part = pl.ds(pl.multiple_of(step % blocks * FIELD_BLOCK, FIELD_BLOCK), FIELD_BLOCK)
        t = (base[0] * tiles[1] + base[1]) * tiles[2] + base[2]
        place_y = wrap(base[1] + along_y, wraps[1])

        def plane(along_x, acc):
            acc = list(acc)
            place_x = wrap(base[0] + along_x, wraps[0])
            for along_z in (-1, 0, 1):
                place = (place_x, place_y, wrap(base[2] + along_z, wraps[2]))
                moment = source_rows(held, place, range(rows))
                k = 9 * (along_x + 1) + 3 * (along_y + 1) + along_z + 1
                d = direct[t, k, part, :]
                away = [apart[i, t, k, part, :] for i in range(3)]
                drawn = [pull[i, t, k, part, :] for i in range(3)]
                for s in range(rows // 3):
                    m = moment[3 * s : 3 * s + 3]
                    project = away[0] * m[0] + away[1] * m[1] + away[2] * m[2]
                    for i in range(3):
                        acc[3 * s + i] = acc[3 * s + i] + (project * drawn[i] - d * m[i])
            return tuple(acc)

        acc = lax.fori_loop(
            -1, 2, plane, tuple(sums[index * count + t, c, part, :] for c in range(rows))
        )
        for c in range(rows):
            sums[index * count + t, c, part, :] = acc[c]

    flat = tiles[0] * tiles[2] * blocks

    def to_row(held, index, row):
        def one(step, carry):
            column = step // blocks % (tiles[0] * tiles[2])
            base = (column // tiles[2], row, column % tiles[2])
            add_sources(held, index, step, base, step // flat - 1)
            return carry

        lax.fori_loop(0, 3 * flat, one, 0)

    def from_row(held, index, row):
        def one(step, carry):
            column = step // blocks % (tiles[0] * tiles[2])
            along_y = step // flat - 1
            base = (column // tiles[2], (row - along_y + tiles[1]) % tiles[1], column % tiles[2])
            add_sources(held, index, step, base, along_y)
            return carry

        lax.fori_loop(0, 3 * flat, one, 0)

    square_lane = lax.broadcasted_iota(jnp.int32, (slots, slots), 1)

    def field_of(index, t):
        columns = jnp.zeros((slots, slots), jnp.float32)
        for c in range(rows):
            value = jnp.sum(sums[index * count + t, c], axis=1, keepdims=True)
            columns = jnp.where(square_lane == c, value, columns)
        return columns.T[0:ROWS]

    for copy in one_copies:
        copy.wait()
    two_copies = []
    for row in range(tiles[1]):
        to_row(held_one, 0, row)
        for t, (x, y, z) in enumerate(places):
            if y == row:
                held_two[x, y, z] = (1.0 - RELAXATION) * held_one[x, y, z] + scaled[t] * (
                    fixed[t] + field_of(0, t)
                )
        copies = halo(held_two, send_two.at[row], recv_two.at[row], row_moves(devices, tiles, row))
        for copy in copies:
            copy.start()
        two_copies.append(copies)
    for row in range(tiles[1]):
        for copy in two_copies[row]:
            copy.wait()
        from_row(held_two, 1, row)
    fields = [field_of(1, t) for t in range(count)]
    changed = jnp.zeros((ROWS, slots), jnp.float32)
    size = jnp.zeros((ROWS, slots), jnp.float32)
    for t, (x, y, z) in enumerate(places):
        before = held_two[x, y, z]
        after = (1.0 - RELAXATION) * before + scaled[t] * (fixed[t] + fields[t])
        for c in range(rows):
            out_ref[c, x, y, z, :] = after[c]
        changed = changed + (after - before) * (after - before)
        size = size + after * after

    def all_of(value):
        return jnp.sum(jnp.sum(value, axis=0, keepdims=True), axis=1, keepdims=True)

    pair = jnp.where(lane == 0, all_of(changed), jnp.where(lane == 1, all_of(size), 0.0))
    slots_b[pl.ds(me, 1)] = pair.reshape(1, 1, slots)
    everyone(1, slots_b)
    everyone_wait(1, slots_b)
    pair = jnp.sum(slots_b[...], axis=0)
    above = jnp.sum(jnp.where(lane == 0, pair, 0.0), axis=1, keepdims=True)
    below = jnp.sum(jnp.where(lane == 1, pair, 0.0), axis=1, keepdims=True)
    change_ref[...] = jnp.broadcast_to(jnp.sqrt(above / (below + 1.0)), (1, slots))


def solution(mesh):
    devices = tuple(mesh.shape[axis] for axis in AXES)
    total_devices = devices[0] * devices[1] * devices[2]

    def on_device(fractions, polarizability, occupancy, pair_mask, perm_field, history):
        tiles = fractions.shape[1:4]
        slots = fractions.shape[4]
        count = tiles[0] * tiles[1] * tiles[2]
        wraps = tuple(n + 2 for n in tiles)
        moves = len(halo_moves(devices, tiles))
        rows = history.shape[1]
        vmem = pl.BlockSpec(memory_space=pltpu.VMEM)
        f32 = jnp.float32
        induced, change = pl.pallas_call(
            functools.partial(kernel, devices),
            out_shape=(
                jax.ShapeDtypeStruct(perm_field.shape, f32),
                jax.ShapeDtypeStruct((1, slots), f32),
            ),
            in_specs=[pl.BlockSpec(memory_space=pltpu.HBM)] * 6,
            out_specs=(vmem, vmem),
            scratch_shapes=[
                pltpu.VMEM(fractions.shape, f32),
                pltpu.VMEM(polarizability.shape, f32),
                pltpu.VMEM(occupancy.shape, jnp.int32),
                pltpu.SMEM(pair_mask.shape, jnp.int32),
                pltpu.VMEM(perm_field.shape, f32),
                pltpu.VMEM(history.shape, f32),
                pltpu.VMEM(wraps + (ROWS, slots), f32),
                pltpu.VMEM(wraps + (ROWS, slots), f32),
                pltpu.VMEM(wraps + (ROWS, slots), f32),
                pltpu.VMEM((history.shape[0], count, ROWS, slots), f32),
                pltpu.VMEM((count, 4, slots, slots), f32),
                pltpu.VMEM((3, count, 27, slots, slots), f32),
                pltpu.VMEM((3, count, 27, slots, slots), f32),
                pltpu.VMEM((count, 27, slots, slots), f32),
                pltpu.VMEM((2 * count, rows, slots, slots), f32),
                pltpu.VMEM((total_devices, 1, slots), f32),
                pltpu.VMEM((total_devices, 1, slots), f32),
                pltpu.SemaphoreType.DMA((6,)),
                pltpu.SemaphoreType.DMA((2,)),
                pltpu.SemaphoreType.DMA((2,)),
            ]
            + [pltpu.SemaphoreType.DMA((moves,))] * 4
            + [pltpu.SemaphoreType.DMA((tiles[1], moves))] * 2,
            compiler_params=pltpu.CompilerParams(
                collective_id=0, has_side_effects=True, vmem_limit_bytes=67043328
            ),
        )(fractions, polarizability, occupancy, pair_mask, perm_field, history)
        return induced, change[0, 0]

    in_specs = (
        P(None, "gx", "gy", "gz", None),
        P("gx", "gy", "gz", None),
        P("gx", "gy", "gz", None),
        P("gx", "gy", "gz", None),
        P(None, "gx", "gy", "gz", None),
        P(None, None, "gx", "gy", "gz", None),
    )
    out_specs = (P(None, "gx", "gy", "gz", None), P())
    return jax.shard_map(
        on_device, mesh=mesh, in_specs=in_specs, out_specs=out_specs, check_vma=False
    )
```
